512 devices in a mesh: dp: 64 (over z, y), tensor: 8 (over x, core).
Axes of the slice: x: 4, y: 4, z: 16, core: 2. Of those that a mesh axis runs over, the one named last changes fastest.
Arguments:
- normed_input: bfloat16 [8192, 8192], P('dp', 'tensor'), may hold values from -6 to 6
- key_cotangent: bfloat16 [8192, 1024], P('dp', 'tensor'), may hold values from -6 to 6
- frozen_key_weight: bfloat16 [8192, 1024], P(None, 'tensor'), may hold values from -0.1875 to 0.1875
- adapter_down_maps: bfloat16 [32, 8192, 16], P(None, 'tensor'), may hold values from -0.0625 to 0.0625
- adapter_up_maps: bfloat16 [32, 16, 1024], P(None, None, 'tensor'), may hold values from -0.1875 to 0.1875
- document_of_token: int32 [8192], P('dp'), may hold values from 0 to 127, never falling along the last dimension, each value on 1 to 512 neighbouring positions
- tenant_of_document: int32 [128], replicated, may hold values from 0 to 31
- tenant_slot_index: int32 [32], replicated, may hold values from 0 to 31, each once
Outputs:
- input_gradient: bfloat16 [8192, 8192], P('dp', 'tensor')
- down_gradient: bfloat16 [32, 8192, 16], P(None, 'tensor')
- up_gradient: bfloat16 [32, 16, 1024], P(None, None, 'tensor')
The draws below stay inside these ranges and needn't reach their ends.
Inputs may be any that keep to these rules, and one draw needn't show every extreme that they name: `document_of_token`: never falling along the tokens; each document 1 to (512) tokens. `tenant_slot_index`: each slot once.
All inputs are finite; a program needn't handle non-finite values.
Results may differ from the reference program's by a relative error of at most 0.008.
Values may be sent and summed in bfloat16 or wider, within the bound.
No kernel may reach another device: no remote copies, remote signals or barrier semaphores. Data moves between devices by JAX's collectives and lax.ppermute only.
A program may use at most 64 MiB of HBM per device.

```python
import math
import jax
import jax.numpy as jnp
import numpy as np

MODEL_WIDTH = 8192
KEY_WIDTH = 1024
ADAPTER_RANK = 16
TENANT_COUNT = 32
TOK_DEV = 128
TOKENS = 8192
DOCS = 128


def touch_ends(values, own_key, low, high):
    spot = [jax.random.randint(jax.random.fold_in(own_key, axis), (), 0, length) for axis, length in enumerate(values.shape)]
    main_axis = values.shape.index(max(values.shape))
    next_to = spot[:main_axis] + [(spot[main_axis] + 1) % values.shape[main_axis]] + spot[main_axis + 1:]
    return values.at[tuple(spot)].set(low).at[tuple(next_to)].set(high)


def block_scale(key, dims, shards, low, high):
    def one(axis_at, shards_of):
        heights = jax.random.uniform(jax.random.fold_in(jax.random.fold_in(key, 6), axis_at), (shards_of,), jnp.float32, low / len(shards), high / len(shards))
        return jnp.repeat(jnp.exp(heights), dims[axis_at] // shards_of).reshape((-1,) + (1,) * (len(dims) - axis_at - 1))

    loudness = one(*shards[0])
    for cut in shards[1:]:
        loudness = loudness * one(*cut)
    return loudness


def rank_table(count, slope):
    weights = [(1 << 20) // math.isqrt(grade ** slope) + 1 for grade in range(1, count + 1)]
    scale = 1 + sum(weights) // (1 << 30)
    return np.cumsum(np.array([max(1, weight // scale) for weight in weights]))


def ranked(own_key, extent, number_of, lean):
    table = rank_table(number_of, lean)
    ticket = jax.random.randint(jax.random.fold_in(own_key, 1), extent, 0, int(table[number_of - 1]))
    grade = jnp.searchsorted(jnp.asarray(table, jnp.int32), ticket, side="right")
    return jax.random.permutation(jax.random.fold_in(own_key, 2), number_of)[grade].astype(jnp.int32)


def profile(number_of, total, most, slope):
    weights = [(1 << 20) // math.isqrt(rank ** slope) + 1 for rank in range(2, number_of + 1)]
    rest, given = total - most - (number_of - 1), [1] * (number_of - 1)
    while rest > 0:
        movable = [i for i in range(number_of - 1) if given[i] < most]
        whole, left = sum([weights[i] for i in movable]), rest
        for i in movable:
            extra = min(most - given[i], max(1, left * weights[i] // whole), rest)
            given[i] = given[i] + extra
            rest = rest - extra
    return np.array([most] + given)


def ragged_sizes(rng, number_of, total, bound, slope):
    if number_of == 2:
        one = jax.random.randint(rng, (), max(1, total - bound), min(bound, total - 1) + 1)
        return jnp.stack([one, total - one])
    sizes = jnp.asarray(profile(number_of, total, bound, slope), jnp.int32)
    twos = (number_of - 1) // 2
    giver, receiver = sizes[1:1 + 2 * twos:2], sizes[2:2 + 2 * twos:2]
    room = jnp.minimum(giver - 1, bound - receiver)
    shifted = jax.random.randint(jax.random.fold_in(rng, 1), (twos,), 0, 1 << 20) % (room + 1)
    sizes = sizes.at[1:1 + 2 * twos:2].set(giver - shifted).at[2:2 + 2 * twos:2].set(receiver + shifted)
    return sizes[jax.random.permutation(jax.random.fold_in(rng, 2), number_of)]


def gaussian(own_key, dims, deviation, most, split=(), held_as=jnp.bfloat16):
    level = block_scale(own_key, dims, split, -0.22, 0.18) if split else 1.0
    values = jax.random.normal(own_key, dims, jnp.float32) * deviation * level
    return jnp.minimum(jnp.maximum(values, -most), most).astype(held_as)


def setup_inputs(seed: int = 0) -> dict:
    seeds = jax.random.split(jax.random.key(seed), 9)
    return {
        "normed_input": gaussian(seeds[0], (TOKENS, MODEL_WIDTH), 1.0, 6.0, ((0, 64), (1, 8))),
        "key_cotangent": gaussian(seeds[1], (TOKENS, KEY_WIDTH), 1.0, 6.0, ((0, 64), (1, 8))),
        "frozen_key_weight": gaussian(seeds[2], (MODEL_WIDTH, KEY_WIDTH), KEY_WIDTH ** -0.5, 0.1875, ((1, 8),)),
        "adapter_down_maps": gaussian(seeds[3], (TENANT_COUNT, MODEL_WIDTH, ADAPTER_RANK), MODEL_WIDTH ** -0.5, 0.0625, ((1, 8),)),
        "adapter_up_maps": gaussian(seeds[4], (TENANT_COUNT, ADAPTER_RANK, KEY_WIDTH), KEY_WIDTH ** -0.5, 0.1875, ((2, 8),)),
        "document_of_token": jnp.searchsorted(jnp.cumsum(ragged_sizes(seeds[5], DOCS, TOKENS, 4 * TOK_DEV, 2)), jnp.arange(TOKENS), side="right").astype(jnp.int32),
        "tenant_of_document": touch_ends(ranked(seeds[6], (DOCS,), TENANT_COUNT, 2), jax.random.fold_in(seeds[6], 3), 0, TENANT_COUNT - 1).astype(jnp.int32),
        "tenant_slot_index": jax.random.permutation(seeds[7], TENANT_COUNT).astype(jnp.int32),
    }


adapter_scale = 2.0


def reference(normed_input, key_cotangent, frozen_key_weight, adapter_down_maps, adapter_up_maps, document_of_token, tenant_of_document, tenant_slot_index):
    tenant_count, model_width, adapter_rank = adapter_down_maps.shape
    slot = jnp.take(tenant_slot_index, jnp.take(tenant_of_document, document_of_token))
    member = (slot[:, None] == jnp.arange(tenant_count, dtype=jnp.int32)[None, :]).astype(jnp.float32)
    down_flattened = jnp.transpose(adapter_down_maps, (1, 0, 2)).reshape(model_width, tenant_count * adapter_rank)
    up_flattened = jnp.transpose(adapter_up_maps, (2, 0, 1)).reshape(adapter_up_maps.shape[2], tenant_count * adapter_rank)
    h_all = jnp.dot(normed_input, down_flattened, preferred_element_type=jnp.float32).reshape(-1, tenant_count, adapter_rank)
    g_all = jnp.dot(key_cotangent, up_flattened, preferred_element_type=jnp.float32).reshape(-1, tenant_count, adapter_rank)
    low_h = jnp.sum(h_all * member[:, :, None], axis=1).astype(jnp.bfloat16)
    low_g = jnp.sum(g_all * member[:, :, None], axis=1).astype(jnp.bfloat16)
    spread_hidden = (member[:, :, None] * low_h.astype(jnp.float32)[:, None, :]).astype(jnp.bfloat16).reshape(-1, tenant_count * adapter_rank)
    spread_cotangent = (member[:, :, None] * low_g.astype(jnp.float32)[:, None, :]).astype(jnp.bfloat16).reshape(-1, tenant_count * adapter_rank)
    frozen_output = jnp.dot(key_cotangent, frozen_key_weight.T, preferred_element_type=jnp.float32)
    adapter_output = jnp.dot(spread_cotangent, down_flattened.T, preferred_element_type=jnp.float32)
    input_gradient = (frozen_output + adapter_scale * adapter_output).astype(jnp.bfloat16)
    down_gradient = adapter_scale * jnp.dot(normed_input.T, spread_cotangent, preferred_element_type=jnp.float32)
    down_gradient = jnp.transpose(down_gradient.reshape(model_width, tenant_count, adapter_rank), (1, 0, 2)).astype(jnp.bfloat16)
    up_gradient = adapter_scale * jnp.dot(spread_hidden.T, key_cotangent, preferred_element_type=jnp.float32)
    up_gradient = up_gradient.reshape(tenant_count, adapter_rank, -1).astype(jnp.bfloat16)
    return input_gradient, down_gradient, up_gradient
```

```python
import jax
import jax.numpy as jnp
from jax import lax
from jax.experimental import pallas as pl
from jax.experimental.pallas import tpu as pltpu
from jax.sharding import Mesh, PartitionSpec as P

adapter_scale = 2.0

Z, Y, T = 16, 4, 8
SLOTS, RANK = 32, 16
ROWS = SLOTS * RANK
bf16, f32 = jnp.bfloat16, jnp.float32
NT = (((1,), (1,)), ((), ()))


def call(body, outs, flops=0, **kw):
    return pl.pallas_call(
        body,
        out_shape=[jax.ShapeDtypeStruct(s, d) for s, d in outs],
        cost_estimate=pl.CostEstimate(flops=flops, bytes_accessed=0, transcendentals=0),
        **kw,
    )


def members(slot):
    return lax.broadcasted_iota(jnp.int32, (ROWS, slot.shape[1]), 0) // RANK == slot


def spread(low, member):
    return jnp.where(member, jnp.concatenate([low] * SLOTS, axis=0), 0.0)


def partial_kernel(x, c, down, up, doc, tenant, index, pack, part, slot_out):
    n = x.shape[0]
    tenant_of = (lax.broadcasted_iota(jnp.int32, (SLOTS, tenant.shape[1]), 0) == tenant[...]).astype(bf16)
    table = jnp.broadcast_to(index[...].astype(f32), (8, SLOTS)).astype(bf16)
    slot_of_doc = jnp.dot(table, tenant_of, preferred_element_type=f32).astype(bf16)
    doc_of = (lax.broadcasted_iota(jnp.int32, (tenant.shape[1], n), 0) == doc[...]).astype(bf16)
    slot = jnp.dot(slot_of_doc, doc_of, preferred_element_type=f32)
    slot_out[...] = slot
    member = members(slot[:1].astype(jnp.int32))
    xt = x[...].astype(f32).T
    ct = c[...].astype(f32).T
    h_all = jnp.dot(down[...], xt.astype(bf16), preferred_element_type=f32)
    g_all = jnp.dot(up[...], ct.astype(bf16), preferred_element_type=f32)
    g = jnp.sum(jnp.where(member, g_all, 0.0).reshape(SLOTS, RANK, n), axis=0)
    h = jnp.sum(jnp.where(member, h_all, 0.0).reshape(SLOTS, RANK, n), axis=0)
    both = jnp.concatenate([g, h], axis=0)
    for i in range(T):
        part[i] = both
    fx, fc = xt.shape[0] // Z, ct.shape[0] // Z
    for z in range(Z):
        pack[z] = jnp.concatenate(
            [xt[z * fx : (z + 1) * fx], ct[z * fc : (z + 1) * fc], slot], axis=0
        ).astype(bf16)


def low_kernel(parts, low, mine):
    total = jnp.sum(parts[...], axis=0).astype(bf16)
    mine[...] = total
    for z in range(Z):
        low[z] = total


def gradient_kernel(pack, low, out):
    fx, fc = 64, 8
    xs, cs, gs, hs = [], [], [], []
    for z in range(Z):
        block = pack[z].astype(f32)
        member = members(block[fx + fc : fx + fc + 1].astype(jnp.int32))
        both = low[z].astype(f32)
        xs.append(block[:fx].astype(bf16))
        cs.append(block[fx : fx + fc].astype(bf16))
        gs.append(spread(both[:RANK], member).astype(bf16))
        hs.append(spread(both[RANK:], member).astype(bf16))
    cat = lambda v: jnp.concatenate(v, axis=1)
    down = lax.dot_general(cat(xs), cat(gs), NT, preferred_element_type=f32)
    up = lax.dot_general(cat(cs), cat(hs), NT, preferred_element_type=f32)
    both = jnp.concatenate([down, up], axis=0)
    rows = ROWS // Y
    for y in range(Y):
        out[y] = both[:, y * rows : (y + 1) * rows]


def finish_kernel(parts, out):
    total = (adapter_scale * jnp.sum(parts[...], axis=0)).astype(bf16)
    for z in range(Z):
        out[z] = total


def layout_kernel(parts, out):
    fx = 64
    v = parts[...].astype(f32)
    down = v[:, :fx].reshape(-1, v.shape[2]).T
    up = v[:, fx:].reshape(-1, v.shape[2]).T
    both = jnp.concatenate([down, up], axis=1).astype(bf16)
    for y in range(Y):
        out[y] = both


def frozen_kernel(c, w, out):
    out[0] = lax.dot_general(c[...], w[...], NT, preferred_element_type=f32).astype(bf16)


def input_kernel(parts, low, slot, down, out):
    g = low[...].astype(f32)[:RANK]
    s = spread(g, members(slot[:1].astype(jnp.int32))).T.astype(bf16)
    adapter = jnp.dot(s, down[...], preferred_element_type=f32)
    frozen = jnp.sum(parts[...].astype(f32), axis=0)
    out[...] = (frozen + adapter_scale * adapter).astype(bf16)


def swap(value, axis):
    return lax.all_to_all(value, axis, 0, 0, tiled=True)


def per_device(x, c, w, down, up, doc, tenant, index):
    n, fx = x.shape
    fc = c.shape[1]
    down_rows = jnp.transpose(down, (0, 2, 1)).reshape(ROWS, fx)
    up_rows = up.reshape(ROWS, fc)
    pack, part, slot = call(
        partial_kernel, [((Z, 80, n), bf16), ((T, 32, n), f32), ((8, n), f32)], flops=10**9
    )(x, c, down_rows, up_rows, doc[None], tenant[None], index[None])
    parts = swap(part, "tensor")
    packs = swap(pack, "z")
    low, mine = call(low_kernel, [((Z, 32, n), bf16), ((32, n), bf16)])(parts)
    lows = swap(low, "z")
    (frozen,) = call(
        frozen_kernel,
        [((T, n, fx), bf16)],
        flops=2 * n * fc * fx * T,
        grid=(T,),
        in_specs=[pl.BlockSpec((n, fc), lambda i: (0, 0)), pl.BlockSpec((fx, fc), lambda i: (i, 0))],
        out_specs=[pl.BlockSpec((1, n, fx), lambda i: (i, 0, 0))],
    )(c, w)
    frozens = swap(frozen, "tensor")
    (piece,) = call(gradient_kernel, [((Y, 72, ROWS // Y), f32)], flops=2 * 2048 * 512 * 512)(packs, lows)
    (mine_out,) = call(finish_kernel, [((Z, 72, ROWS // Y), bf16)])(swap(piece, "y"))
    (block,) = call(layout_kernel, [((Y, ROWS // Y, fx + fc), bf16)])(swap(mine_out, "z"))
    (input_gradient,) = call(input_kernel, [((n, fx), bf16)], flops=10**9)(frozens, mine, slot, down_rows)
    whole = swap(block, "y").reshape(ROWS, fx + fc)
    down_gradient = jnp.transpose(whole[:, :fx].reshape(SLOTS, RANK, fx), (0, 2, 1))
    up_gradient = whole[:, fx:].reshape(SLOTS, RANK, fc)
    return input_gradient, down_gradient, up_gradient


def solution(mesh):
    grid = Mesh(mesh.devices.reshape(Z, Y, T), ("z", "y", "tensor"))
    dp = ("z", "y")
    in_specs = (
        P(dp, "tensor"),
        P(dp, "tensor"),
        P(None, "tensor"),
        P(None, "tensor", None),
        P(None, None, "tensor"),
        P(dp),
        P(),
        P(),
    )
    out_specs = (P(dp, "tensor"), P(None, "tensor", None), P(None, None, "tensor"))
    return jax.shard_map(
        per_device, mesh=grid, in_specs=in_specs, out_specs=out_specs, check_vma=False
    )
```

```python
import jax
import jax.numpy as jnp
from jax import lax
from jax.experimental import pallas as pl
from jax.experimental.pallas import tpu as pltpu
from jax.sharding import Mesh, PartitionSpec as P

adapter_scale = 2.0

Z, Y, T = 16, 4, 8
SLOTS, RANK = 32, 16
ROWS = SLOTS * RANK
bf16, f32 = jnp.bfloat16, jnp.float32
NT = (((1,), (1,)), ((), ()))


def call(body, outs, flops=0, **kw):
    return pl.pallas_call(
        body,
        out_shape=[jax.ShapeDtypeStruct(s, d) for s, d in outs],
        cost_estimate=pl.CostEstimate(flops=flops, bytes_accessed=0, transcendentals=0),
        **kw,
    )


def spread(low, slot, first=0, slots=SLOTS):
    at = lax.broadcasted_iota(jnp.int32, (slots * RANK, low.shape[1]), 0) // RANK + first
    return jnp.where(at == slot, jnp.concatenate([low] * slots, axis=0), 0.0)


def partial_kernel(x, c, down, up, doc, tenant, index, me, pack, part, slot_out):
    n = x.shape[0]
    tenant_of = (lax.broadcasted_iota(jnp.int32, (SLOTS, tenant.shape[1]), 0) == tenant[...]).astype(bf16)
    table = jnp.broadcast_to(index[...].astype(f32), (8, SLOTS)).astype(bf16)
    slot_of_doc = jnp.dot(table, tenant_of, preferred_element_type=f32).astype(bf16)
    doc_of = (lax.broadcasted_iota(jnp.int32, (tenant.shape[1], n), 0) == doc[...]).astype(bf16)
    slot = jnp.dot(slot_of_doc, doc_of, preferred_element_type=f32)
    slot_out[...] = slot
    member = lax.broadcasted_iota(jnp.int32, (ROWS, n), 0) // RANK == slot[:1].astype(jnp.int32)
    h_all = lax.dot_general(down[...], x[...], NT, preferred_element_type=f32)
    g_all = lax.dot_general(up[...], c[...], NT, preferred_element_type=f32)
    g = jnp.sum(jnp.where(member, g_all, 0.0).reshape(SLOTS, RANK, n), axis=0)
    h = jnp.sum(jnp.where(member, h_all, 0.0).reshape(SLOTS, RANK, n), axis=0)
    both = jnp.concatenate([g, h], axis=0)
    for i in range(Y * T):
        part[i] = both
    fx = x.shape[1] // Y
    slots = jnp.concatenate([slot, jnp.zeros((8, pack.shape[2] - n), f32)], axis=1)
    for y in range(Y):
        mine = jnp.concatenate([x[:, y * fx : (y + 1) * fx], c[...]], axis=1)
        pack[(y - me[0]) & (Y - 1)] = jnp.concatenate([mine.astype(f32), slots], axis=0).astype(bf16)


def gradient_kernel(me, parts, p0, p1, p2, p3, out, low_out):
    fx = p0.shape[1] - 128
    gs, hs = [], []
    for k, pack in enumerate((p0, p1, p2, p3)):
        at = (me[0] - k) & (Y - 1)
        both = parts[at * T]
        for j in range(1, T):
            both = both + parts[at * T + j]
        both = both.astype(bf16)
        if k == 0:
            low_out[...] = both
        both = both.astype(f32)
        slot = pack[128:, :128].astype(f32)[:1].astype(jnp.int32)
        gs.append(spread(both[:RANK], slot).astype(bf16))
        hs.append(spread(both[RANK:], slot, me[0] * (SLOTS // Y), SLOTS // Y).astype(bf16))
    xs = jnp.concatenate([p[:128, :fx] for p in (p0, p1, p2, p3)], axis=0)
    cs = jnp.concatenate([p[:128, fx:] for p in (p0, p1, p2, p3)], axis=0)
    down = jnp.dot(jnp.concatenate(gs, axis=1), xs, preferred_element_type=f32)
    up = jnp.dot(jnp.concatenate(hs, axis=1), cs, preferred_element_type=f32)
    rd, ru = ROWS // Z, ROWS // Y // Z
    for z in range(Z):
        one = down[z * rd : (z + 1) * rd]
        out[z] = jnp.concatenate([one[:, :128], one[:, 128:], up[z * ru : (z + 1) * ru]], axis=0).astype(bf16)


def finish_kernel(parts, out):
    total = (adapter_scale * jnp.sum(parts[...].astype(f32), axis=0)).astype(bf16)
    for z in range(Z):
        out[z] = total


def layout_kernel(me, g0, g1, g2, g3, down, up):
    rd = ROWS // Z
    for k, g in enumerate((g0, g1, g2, g3)):
        at = (me[0] - k) & (Y - 1)
        v = g[...].astype(f32)
        down[:, pl.ds(pl.multiple_of(at * 256, 256), 128)] = v[:, :rd].reshape(ROWS, 128).astype(bf16)
        down[:, pl.ds(pl.multiple_of(at * 256 + 128, 128), 128)] = v[:, rd : 2 * rd].reshape(ROWS, 128).astype(bf16)
        up[pl.ds(pl.multiple_of(at * 128, 128), 128)] = v[:, 2 * rd :].reshape(128, 128).astype(bf16)


def frozen_kernel(where, c, w, out):
    out[0] = lax.dot_general(c[...], w[...], NT, preferred_element_type=f32).astype(bf16)


def pair_kernel(kept, came, o0, o1, o2, o3):
    for k, out in enumerate((o0, o1, o2, o3)):
        out[...] = (kept[k].astype(f32) + came[k].astype(f32)).astype(bf16)


def input_kernel(f0, f1, f2, f3, low, slot, down, out):
    g = low[...].astype(f32)[:RANK]
    s = spread(g, slot[:1].astype(jnp.int32)).T.astype(bf16)
    adapter = jnp.dot(s, down[...], preferred_element_type=f32)
    frozen = (f0[...].astype(f32) + f1[...].astype(f32)) + (f2[...].astype(f32) + f3[...].astype(f32))
    out[...] = (frozen + adapter_scale * adapter).astype(bf16)


def swap(value, axis):
    return lax.all_to_all(value, axis, 0, 0, tiled=True)


def shift(value, axis, by):
    size = lax.axis_size(axis)
    return lax.ppermute(value, axis, [(i, (i + by) % size) for i in range(size)])


def specs(count):
    return [pl.BlockSpec(memory_space=pltpu.SMEM)] + [pl.BlockSpec(memory_space=pltpu.VMEM)] * count


def frozen_blocks(c, w, place):
    n, fc = c.shape
    fx = w.shape[0] // T
    return pl.pallas_call(
        frozen_kernel,
        grid_spec=pltpu.PrefetchScalarGridSpec(
            num_scalar_prefetch=1,
            grid=(4,),
            in_specs=[
                pl.BlockSpec((n, fc), lambda i, p: (0, 0)),
                pl.BlockSpec((fx, fc), lambda i, p: (((p[0] + i) & 3) * 2 + p[1], 0)),
            ],
            out_specs=pl.BlockSpec((1, n, fx), lambda i, p: (i, 0, 0)),
        ),
        out_shape=jax.ShapeDtypeStruct((4, n, fx), bf16),
        cost_estimate=pl.CostEstimate(flops=10**9, bytes_accessed=0, transcendentals=0),
    )(place, c, w)


def per_device(x, c, w, down, up, doc, tenant, index):
    n, fx = x.shape
    fc = c.shape[1]
    me = lax.axis_index("y")[None]
    at = lax.axis_index("tensor")
    down_rows = jnp.transpose(down, (0, 2, 1)).reshape(ROWS, fx)
    up_rows = up.reshape(ROWS, fc)
    block = (ROWS // Z * 2 + ROWS // Y // Z, 128)
    pack, part, slot = call(
        partial_kernel,
        [((Y, n + 8, fx // Y + fc), bf16), ((Y * T, 2 * RANK, n), f32), ((8, n), f32)],
        flops=10**9,
        in_specs=[pl.BlockSpec(memory_space=pltpu.VMEM)] * 7 + [pl.BlockSpec(memory_space=pltpu.SMEM)],
    )(x, c, down_rows, up_rows, doc[None], tenant[None], index[None], me)
    parts = swap(part, ("y", "tensor"))
    packs = [pack[0]]
    for k in (1, 2, 3):
        packs.append(shift(pack[k], "y", k))
    piece, low = call(
        gradient_kernel,
        [((Z, *block), bf16), ((2 * RANK, n), bf16)],
        flops=10**9,
        in_specs=specs(5),
    )(me, parts, *packs)
    sums = swap(piece, "z")
    send = frozen_blocks(c, w, jnp.stack([at // 2, 1 - at % 2]))
    came = lax.ppermute(send, "tensor", [(j, j ^ 1) for j in range(T)])
    kept = frozen_blocks(c, w, jnp.stack([at // 2, at % 2]))
    pairs = call(pair_kernel, [((n, fx), bf16)] * 4, flops=10**8)(kept, came)
    frozens = [pairs[0]]
    for k in (1, 2, 3):
        frozens.append(shift(pairs[k], "tensor", 2 * k))
    (done,) = call(finish_kernel, [((Z, *block), bf16)], flops=10**8)(sums)
    rows = swap(done, "z")
    (input_gradient,) = call(input_kernel, [((n, fx), bf16)], flops=10**9)(*frozens, low, slot, down_rows)
    outs = [rows]
    for k in (1, 2, 3):
        outs.append(shift(rows, "y", k))
    whole, up_whole = call(layout_kernel, [((ROWS, fx), bf16), ((ROWS, fc), bf16)], in_specs=specs(4))(me, *outs)
    down_gradient = jnp.transpose(whole.reshape(SLOTS, RANK, fx), (0, 2, 1))
    up_gradient = up_whole.reshape(SLOTS, RANK, fc)
    return input_gradient, down_gradient, up_gradient


def solution(mesh):
    grid = Mesh(mesh.devices.reshape(Z, Y, T), ("z", "y", "tensor"))
    dp = ("z", "y")
    in_specs = (
        P(dp, "tensor"),
        P(dp, "tensor"),
        P(None, "tensor"),
        P(None, "tensor", None),
        P(None, None, "tensor"),
        P(dp),
        P(),
        P(),
    )
    out_specs = (P(dp, "tensor"), P(None, "tensor", None), P(None, None, "tensor"))

    return jax.shard_map(per_device, mesh=grid, in_specs=in_specs, out_specs=out_specs, check_vma=False)
```

```python
import jax
import jax.numpy as jnp
from jax import lax
from jax.experimental import pallas as pl
from jax.experimental.pallas import tpu as pltpu
from jax.sharding import Mesh, PartitionSpec as P

adapter_scale = 2.0

Z, Y, T = 16, 4, 8
SLOTS, RANK = 32, 16
ROWS = SLOTS * RANK
bf16, f32 = jnp.bfloat16, jnp.float32
NT = (((1,), (1,)), ((), ()))


GRANT = pltpu.CompilerParams(vmem_limit_bytes=12 << 20)


def call(body, outs, flops=0, **kw):
    return pl.pallas_call(
        body,
        compiler_params=GRANT,
        out_shape=[jax.ShapeDtypeStruct(s, d) for s, d in outs],
        cost_estimate=pl.CostEstimate(flops=flops, bytes_accessed=0, transcendentals=0),
        **kw,
    )


def spread(low, slot, first=0, slots=SLOTS):
    at = lax.broadcasted_iota(jnp.int32, (slots * RANK, low.shape[1]), 0) // RANK + first
    return jnp.where(at == slot, jnp.concatenate([low] * slots, axis=0), 0.0)


def partial_kernel(x, c, down, up, doc, tenant, index, me, part, slot_out, *packs):
    n = x.shape[0]
    tenant_of = (lax.broadcasted_iota(jnp.int32, (SLOTS, tenant.shape[1]), 0) == tenant[...]).astype(bf16)
    table = jnp.broadcast_to(index[...].astype(f32), (8, SLOTS)).astype(bf16)
    slot_of_doc = jnp.dot(table, tenant_of, preferred_element_type=f32).astype(bf16)
    doc_of = (lax.broadcasted_iota(jnp.int32, (tenant.shape[1], n), 0) == doc[...]).astype(bf16)
    slot = jnp.dot(slot_of_doc, doc_of, preferred_element_type=f32)
    slot_out[...] = slot
    member = lax.broadcasted_iota(jnp.int32, (ROWS, n), 0) // RANK == slot[:1].astype(jnp.int32)
    h_all = lax.dot_general(down[...], x[...], NT, preferred_element_type=f32)
    g_all = lax.dot_general(up[...], c[...], NT, preferred_element_type=f32)
    g = jnp.sum(jnp.where(member, g_all, 0.0).reshape(SLOTS, RANK, n), axis=0)
    h = jnp.sum(jnp.where(member, h_all, 0.0).reshape(SLOTS, RANK, n), axis=0)
    both = jnp.concatenate([g, h], axis=0)
    for i in range(Y * T):
        part[i] = both
    fx = x.shape[1] // Y
    slots = jnp.concatenate([slot, jnp.zeros((8, fx + c.shape[1] - n), f32)], axis=1)
    for k, pack in enumerate(packs):
        at = pl.multiple_of((me[0] ^ k) * fx, fx)
        mine = jnp.concatenate([x[:, pl.ds(at, fx)], c[...]], axis=1)
        pack[...] = jnp.concatenate([mine.astype(f32), slots], axis=0).astype(bf16)


def gradient_kernel(me, parts, p0, p1, p2, p3, out, low_out):
    fx = p0.shape[1] - 128
    gs, hs = [], []
    for k, pack in enumerate((p0, p1, p2, p3)):
        at = me[0] ^ k
        both = parts[at * T]
        for j in range(1, T):
            both = both + parts[at * T + j]
        both = both.astype(bf16)
        if k == 0:
            low_out[...] = both
        both = both.astype(f32)
        slot = pack[128:, :128].astype(f32)[:1].astype(jnp.int32)
        gs.append(spread(both[:RANK], slot).astype(bf16))
        hs.append(spread(both[RANK:], slot, me[0] * (SLOTS // Y), SLOTS // Y).astype(bf16))
    xs = jnp.concatenate([p[:128, :fx] for p in (p0, p1, p2, p3)], axis=0)
    cs = jnp.concatenate([p[:128, fx:] for p in (p0, p1, p2, p3)], axis=0)
    down = jnp.dot(jnp.concatenate(gs, axis=1), xs, preferred_element_type=f32)
    up = jnp.dot(jnp.concatenate(hs, axis=1), cs, preferred_element_type=f32)
    rd, ru = ROWS // Z, ROWS // Y // Z
    for z in range(Z):
        one = down[z * rd : (z + 1) * rd]
        out[z] = jnp.concatenate([one[:, :128], one[:, 128:], up[z * ru : (z + 1) * ru]], axis=0).astype(bf16)


def finish_kernel(parts, out):
    total = (adapter_scale * jnp.sum(parts[...].astype(f32), axis=0)).astype(bf16)
    for z in range(Z):
        out[z] = total


def layout_kernel(me, g0, g1, g2, g3, down, up):
    rd = ROWS // Z
    for k, g in enumerate((g0, g1, g2, g3)):
        at = me[0] ^ k
        v = g[...].astype(f32)
        down[:, pl.ds(pl.multiple_of(at * 256, 256), 128)] = v[:, :rd].reshape(ROWS, 128).astype(bf16)
        down[:, pl.ds(pl.multiple_of(at * 256 + 128, 128), 128)] = v[:, rd : 2 * rd].reshape(ROWS, 128).astype(bf16)
        up[pl.ds(pl.multiple_of(at * 128, 128), 128)] = v[:, 2 * rd :].reshape(128, 128).astype(bf16)


def frozen_kernel(where, c, w, out):
    out[0] = lax.dot_general(c[...], w[...], NT, preferred_element_type=f32).astype(bf16)


def pair_kernel(kept, came, o0, o1, o2, o3):
    for k, out in enumerate((o0, o1, o2, o3)):
        out[...] = (kept[k].astype(f32) + came[k].astype(f32)).astype(bf16)


def input_kernel(f0, f1, f2, f3, low, slot, down, out):
    g = low[...].astype(f32)[:RANK]
    s = spread(g, slot[:1].astype(jnp.int32)).T.astype(bf16)
    adapter = jnp.dot(s, down[...], preferred_element_type=f32)
    frozen = (f0[...].astype(f32) + f1[...].astype(f32)) + (f2[...].astype(f32) + f3[...].astype(f32))
    out[...] = (frozen + adapter_scale * adapter).astype(bf16)


def swap(value, axis):
    return lax.all_to_all(value, axis, 0, 0, tiled=True)


def trade(value, axis, k):
    return lax.ppermute(value, axis, [(i, i ^ k) for i in range(lax.axis_size(axis))])


def specs(count):
    return [pl.BlockSpec(memory_space=pltpu.SMEM)] + [pl.BlockSpec(memory_space=pltpu.VMEM)] * count


def frozen_blocks(c, w, place):
    n, fc = c.shape
    fx = w.shape[0] // T
    return pl.pallas_call(
        frozen_kernel,
        compiler_params=GRANT,
        grid_spec=pltpu.PrefetchScalarGridSpec(
            num_scalar_prefetch=1,
            grid=(4,),
            in_specs=[
                pl.BlockSpec((n, fc), lambda i, p: (0, 0)),
                pl.BlockSpec((fx, fc), lambda i, p: ((p[0] ^ i) * 2 + p[1], 0)),
            ],
            out_specs=pl.BlockSpec((1, n, fx), lambda i, p: (i, 0, 0)),
        ),
        out_shape=jax.ShapeDtypeStruct((4, n, fx), bf16),
        cost_estimate=pl.CostEstimate(flops=10**9, bytes_accessed=0, transcendentals=0),
    )(place, c, w)


def per_device(x, c, w, down, up, doc, tenant, index):
    n, fx = x.shape
    fc = c.shape[1]
    me = lax.axis_index("y")[None]
    at = lax.axis_index("tensor")
    down_rows = jnp.transpose(down, (0, 2, 1)).reshape(ROWS, fx)
    up_rows = up.reshape(ROWS, fc)
    block = (ROWS // Z * 2 + ROWS // Y // Z, 128)
    part, slot, *packs = call(
        partial_kernel,
        [((Y * T, 2 * RANK, n), f32), ((8, n), f32)] + [((n + 8, fx // Y + fc), bf16)] * Y,
        flops=10**9,
        in_specs=[pl.BlockSpec(memory_space=pltpu.VMEM)] * 7 + [pl.BlockSpec(memory_space=pltpu.SMEM)],
    )(x, c, down_rows, up_rows, doc[None], tenant[None], index[None], me)
    parts = swap(part, ("y", "tensor"))
    for k in (1, 2, 3):
        packs[k] = trade(packs[k], "y", k)
    piece, low = call(
        gradient_kernel,
        [((Z, *block), bf16), ((2 * RANK, n), bf16)],
        flops=10**9,
        in_specs=specs(5),
    )(me, parts, *packs)
    sums = swap(piece, "z")
    send = frozen_blocks(c, w, jnp.stack([at >> 1, (at & 1) ^ 1]))
    came = trade(send, "tensor", 1)
    kept = frozen_blocks(c, w, jnp.stack([at >> 1, at & 1]))
    pairs = call(pair_kernel, [((n, fx), bf16)] * 4, flops=10**8)(kept, came)
    frozens = [pairs[0]]
    for k in (1, 2, 3):
        frozens.append(trade(pairs[k], "tensor", 2 * k))
    (done,) = call(finish_kernel, [((Z, *block), bf16)], flops=10**8)(sums)
    rows = swap(done, "z")
    (input_gradient,) = call(input_kernel, [((n, fx), bf16)], flops=10**9)(*frozens, low, slot, down_rows)
    outs = [rows]
    for k in (1, 2, 3):
        outs.append(trade(rows, "y", k))
    whole, up_whole = call(layout_kernel, [((ROWS, fx), bf16), ((ROWS, fc), bf16)], in_specs=specs(4))(me, *outs)
    down_gradient = jnp.transpose(whole.reshape(SLOTS, RANK, fx), (0, 2, 1))
    up_gradient = up_whole.reshape(SLOTS, RANK, fc)
    return input_gradient, down_gradient, up_gradient


def solution(mesh):
    grid = Mesh(mesh.devices.reshape(Z, Y, T), ("z", "y", "tensor"))
    dp = ("z", "y")
    in_specs = (
        P(dp, "tensor"),
        P(dp, "tensor"),
        P(None, "tensor"),
        P(None, "tensor", None),
        P(None, None, "tensor"),
        P(dp),
        P(),
        P(),
    )
    out_specs = (P(dp, "tensor"), P(None, "tensor", None), P(None, None, "tensor"))

    return jax.shard_map(per_device, mesh=grid, in_specs=in_specs, out_specs=out_specs, check_vma=False)
```

```python
import jax
import jax.numpy as jnp
from jax import lax
from jax.experimental import pallas as pl
from jax.experimental.pallas import tpu as pltpu
from jax.sharding import Mesh, PartitionSpec as P

adapter_scale = 2.0

Z, Y, T = 16, 4, 8
SLOTS, RANK = 32, 16
ROWS = SLOTS * RANK
bf16, f32 = jnp.bfloat16, jnp.float32
NT = (((1,), (1,)), ((), ()))


GRANT = pltpu.CompilerParams(vmem_limit_bytes=12 << 20)


def call(body, outs, flops=0, grant=GRANT, **kw):
    return pl.pallas_call(
        body,
        compiler_params=grant,
        out_shape=[pltpu.VMEM(s, d) for s, d in outs],
        cost_estimate=pl.CostEstimate(flops=flops, bytes_accessed=0, transcendentals=0),
        **kw,
    )


def spread(low, slot, first=0, slots=SLOTS):
    at = lax.broadcasted_iota(jnp.int32, (slots * RANK, low.shape[1]), 0) // RANK + first
    return jnp.where(at == slot, jnp.concatenate([low] * slots, axis=0), 0.0)


def partial_kernel(x, c, down, up, doc, tenant, index, me, part, slot_out, *packs):
    n = x.shape[0]
    tenant_of = (lax.broadcasted_iota(jnp.int32, (SLOTS, tenant.shape[1]), 0) == tenant[...]).astype(bf16)
    table = jnp.broadcast_to(index[...].astype(f32), (8, SLOTS)).astype(bf16)
    slot_of_doc = jnp.dot(table, tenant_of, preferred_element_type=f32).astype(bf16)
    doc_of = (lax.broadcasted_iota(jnp.int32, (tenant.shape[1], n), 0) == doc[...]).astype(bf16)
    slot = jnp.dot(slot_of_doc, doc_of, preferred_element_type=f32)
    slot_out[...] = slot
    member = lax.broadcasted_iota(jnp.int32, (ROWS, n), 0) // RANK == slot[:1].astype(jnp.int32)
    h_all = lax.dot_general(down[...], x[...], NT, preferred_element_type=f32)
    g_all = lax.dot_general(up[...], c[...], NT, preferred_element_type=f32)
    g = jnp.sum(jnp.where(member, g_all, 0.0).reshape(SLOTS, RANK, n), axis=0)
    h = jnp.sum(jnp.where(member, h_all, 0.0).reshape(SLOTS, RANK, n), axis=0)
    both = jnp.concatenate([g, h], axis=0)
    for i in range(Y * T):
        part[i] = both
    fx = x.shape[1] // Y
    slots = jnp.concatenate([slot, jnp.zeros((8, fx + c.shape[1] - n), f32)], axis=1)
    for k, pack in enumerate(packs):
        at = pl.multiple_of((me[0] ^ k) * fx, fx)
        mine = jnp.concatenate([x[:, pl.ds(at, fx)], c[...]], axis=1)
        pack[...] = jnp.concatenate([mine.astype(f32), slots], axis=0).astype(bf16)


def gradient_kernel(me, parts, p0, p1, p2, p3, out, low_out):
    fx = p0.shape[1] - 128
    gs, hs = [], []
    for k, pack in enumerate((p0, p1, p2, p3)):
        at = me[0] ^ k
        both = parts[at * T]
        for j in range(1, T):
            both = both + parts[at * T + j]
        both = both.astype(bf16)
        if k == 0:
            low_out[...] = both
        both = both.astype(f32)
        slot = pack[128:, :128].astype(f32)[:1].astype(jnp.int32)
        gs.append(spread(both[:RANK], slot).astype(bf16))
        hs.append(spread(both[RANK:], slot, me[0] * (SLOTS // Y), SLOTS // Y).astype(bf16))
    xs = jnp.concatenate([p[:128, :fx] for p in (p0, p1, p2, p3)], axis=0)
    cs = jnp.concatenate([p[:128, fx:] for p in (p0, p1, p2, p3)], axis=0)
    down = jnp.dot(jnp.concatenate(gs, axis=1), xs, preferred_element_type=f32)
    up = jnp.dot(jnp.concatenate(hs, axis=1), cs, preferred_element_type=f32)
    rd, ru = ROWS // Z, ROWS // Y // Z
    for z in range(Z):
        one = down[z * rd : (z + 1) * rd]
        out[z] = jnp.concatenate([one[:, :128], one[:, 128:], up[z * ru : (z + 1) * ru]], axis=0).astype(bf16)


def finish_kernel(parts, out):
    total = (adapter_scale * jnp.sum(parts[...].astype(f32), axis=0)).astype(bf16)
    for z in range(Z):
        out[z] = total


def layout_kernel(me, g0, g1, g2, g3, down, up):
    rd = ROWS // Z
    for k, g in enumerate((g0, g1, g2, g3)):
        at = me[0] ^ k
        v = g[...].astype(f32)
        down[:, pl.ds(pl.multiple_of(at * 256, 256), 128)] = v[:, :rd].reshape(ROWS, 128).astype(bf16)
        down[:, pl.ds(pl.multiple_of(at * 256 + 128, 128), 128)] = v[:, rd : 2 * rd].reshape(ROWS, 128).astype(bf16)
        up[pl.ds(pl.multiple_of(at * 128, 128), 128)] = v[:, 2 * rd :].reshape(128, 128).astype(bf16)


def frozen_kernel(where, c, w, out):
    out[0] = lax.dot_general(c[...], w[...], NT, preferred_element_type=f32).astype(bf16)


def pair_kernel(kept, came, o0, o1, o2, o3):
    for k, out in enumerate((o0, o1, o2, o3)):
        out[...] = (kept[k].astype(f32) + came[k].astype(f32)).astype(bf16)


def input_kernel(f0, f1, f2, f3, low, slot, down, out):
    g = low[...].astype(f32)[:RANK]
    s = spread(g, slot[:1].astype(jnp.int32)).T.astype(bf16)
    adapter = jnp.dot(s, down[...], preferred_element_type=f32)
    frozen = (f0[...].astype(f32) + f1[...].astype(f32)) + (f2[...].astype(f32) + f3[...].astype(f32))
    out[...] = (frozen + adapter_scale * adapter).astype(bf16)


def swap(value, axis):
    return lax.all_to_all(value, axis, 0, 0, tiled=True)


def trade(value, axis, k):
    return lax.ppermute(value, axis, [(i, i ^ k) for i in range(lax.axis_size(axis))])


def specs(count):
    return [pl.BlockSpec(memory_space=pltpu.SMEM)] + [pl.BlockSpec(memory_space=pltpu.VMEM)] * count


def frozen_blocks(c, w, place):
    n, fc = c.shape
    fx = w.shape[0] // T
    return pl.pallas_call(
        frozen_kernel,
        compiler_params=GRANT,
        grid_spec=pltpu.PrefetchScalarGridSpec(
            num_scalar_prefetch=1,
            grid=(4,),
            in_specs=[
                pl.BlockSpec((n, fc), lambda i, p: (0, 0)),
                pl.BlockSpec((fx, fc), lambda i, p: ((p[0] ^ i) * 2 + p[1], 0)),
            ],
            out_specs=pl.BlockSpec((1, n, fx), lambda i, p: (i, 0, 0)),
        ),
        out_shape=jax.ShapeDtypeStruct((4, n, fx), bf16),
        cost_estimate=pl.CostEstimate(flops=10**9, bytes_accessed=0, transcendentals=0),
    )(place, c, w)


def per_device(x, c, w, down, up, doc, tenant, index):
    n, fx = x.shape
    fc = c.shape[1]
    me = lax.axis_index("y")[None]
    at = lax.axis_index("tensor")
    down_rows = jnp.transpose(down, (0, 2, 1)).reshape(ROWS, fx)
    up_rows = up.reshape(ROWS, fc)
    block = (ROWS // Z * 2 + ROWS // Y // Z, 128)
    part, slot, *packs = call(
        partial_kernel,
        [((Y * T, 2 * RANK, n), f32), ((8, n), f32)] + [((n + 8, fx // Y + fc), bf16)] * Y,
        flops=10**9,
        grant=pltpu.CompilerParams(),
        in_specs=[pl.BlockSpec(memory_space=pltpu.VMEM)] * 7 + [pl.BlockSpec(memory_space=pltpu.SMEM)],
    )(x, c, down_rows, up_rows, doc[None], tenant[None], index[None], me)
    parts = swap(part, ("y", "tensor"))
    for k in (1, 2, 3):
        packs[k] = trade(packs[k], "y", k)
    piece, low = call(
        gradient_kernel,
        [((Z, *block), bf16), ((2 * RANK, n), bf16)],
        flops=10**9,
        in_specs=specs(5),
    )(me, parts, *packs)
    sums = swap(piece, "z")
    send = frozen_blocks(c, w, jnp.stack([at >> 1, (at & 1) ^ 1]))
    came = trade(send, "tensor", 1)
    kept = frozen_blocks(c, w, jnp.stack([at >> 1, at & 1]))
    pairs = call(pair_kernel, [((n, fx), bf16)] * 4, flops=10**8)(kept, came)
    frozens = [pairs[0]]
    for k in (1, 2, 3):
        frozens.append(trade(pairs[k], "tensor", 2 * k))
    (done,) = call(finish_kernel, [((Z, *block), bf16)], flops=10**8)(sums)
    rows = swap(done, "z")
    (input_gradient,) = call(input_kernel, [((n, fx), bf16)], flops=10**9)(*frozens, low, slot, down_rows)
    outs = [rows]
    for k in (1, 2, 3):
        outs.append(trade(rows, "y", k))
    whole, up_whole = call(layout_kernel, [((ROWS, fx), bf16), ((ROWS, fc), bf16)], in_specs=specs(4))(me, *outs)
    down_gradient = jnp.transpose(whole.reshape(SLOTS, RANK, fx), (0, 2, 1))
    up_gradient = up_whole.reshape(SLOTS, RANK, fc)
    return input_gradient, down_gradient, up_gradient


def solution(mesh):
    grid = Mesh(mesh.devices.reshape(Z, Y, T), ("z", "y", "tensor"))
    dp = ("z", "y")
    in_specs = (
        P(dp, "tensor"),
        P(dp, "tensor"),
        P(None, "tensor"),
        P(None, "tensor", None),
        P(None, None, "tensor"),
        P(dp),
        P(),
        P(),
    )
    out_specs = (P(dp, "tensor"), P(None, "tensor", None), P(None, None, "tensor"))

    return jax.shard_map(per_device, mesh=grid, in_specs=in_specs, out_specs=out_specs, check_vma=False)
```

```python
import jax
import jax.numpy as jnp
from jax import lax
from jax.experimental import pallas as pl
from jax.experimental.pallas import tpu as pltpu
from jax.sharding import Mesh, PartitionSpec as P

adapter_scale = 2.0

Z, Y, T = 16, 4, 8
SLOTS, RANK = 32, 16
ROWS = SLOTS * RANK
bf16, f32 = jnp.bfloat16, jnp.float32
NT = (((1,), (1,)), ((), ()))


GRANT = pltpu.CompilerParams(vmem_limit_bytes=12 << 20)


def call(body, outs, flops=0, grant=GRANT, out=pltpu.VMEM, **kw):
    return pl.pallas_call(
        body,
        compiler_params=grant,
        out_shape=[out(s, d) for s, d in outs],
        cost_estimate=pl.CostEstimate(flops=flops, bytes_accessed=0, transcendentals=0),
        **kw,
    )


def spread(low, slot, first=0, slots=SLOTS):
    at = lax.broadcasted_iota(jnp.int32, (slots * RANK, low.shape[1]), 0) // RANK + first
    return jnp.where(at == slot, jnp.concatenate([low] * slots, axis=0), 0.0)


def partial_kernel(x, c, down, up, doc, tenant, index, me, part, slot_out, *packs):
    n = x.shape[0]
    tenant_of = (lax.broadcasted_iota(jnp.int32, (SLOTS, tenant.shape[1]), 0) == tenant[...]).astype(bf16)
    table = jnp.broadcast_to(index[...].astype(f32), (8, SLOTS)).astype(bf16)
    slot_of_doc = jnp.dot(table, tenant_of, preferred_element_type=f32).astype(bf16)
    doc_of = (lax.broadcasted_iota(jnp.int32, (tenant.shape[1], n), 0) == doc[...]).astype(bf16)
    slot = jnp.dot(slot_of_doc, doc_of, preferred_element_type=f32)
    slot_out[...] = slot
    member = lax.broadcasted_iota(jnp.int32, (ROWS, n), 0) // RANK == slot[:1].astype(jnp.int32)
    h_all = lax.dot_general(down[...], x[...], NT, preferred_element_type=f32)
    g_all = lax.dot_general(up[...], c[...], NT, preferred_element_type=f32)
    g = jnp.sum(jnp.where(member, g_all, 0.0).reshape(SLOTS, RANK, n), axis=0)
    h = jnp.sum(jnp.where(member, h_all, 0.0).reshape(SLOTS, RANK, n), axis=0)
    both = jnp.concatenate([g, h], axis=0).astype(bf16)
    for i in range(Y * T):
        part[i] = both
    fx = x.shape[1] // Y
    slots = jnp.concatenate([slot, jnp.zeros((8, fx + c.shape[1] - n), f32)], axis=1)
    for k, pack in enumerate(packs):
        at = pl.multiple_of((me[0] ^ k) * fx, fx)
        mine = jnp.concatenate([x[:, pl.ds(at, fx)], c[...]], axis=1)
        pack[...] = jnp.concatenate([mine.astype(f32), slots], axis=0).astype(bf16)


def gradient_kernel(me, parts, p0, p1, p2, p3, out, low_out):
    fx = p0.shape[1] - 128
    gs, hs = [], []
    for k, pack in enumerate((p0, p1, p2, p3)):
        at = me[0] ^ k
        both = parts[at * T].astype(f32)
        for j in range(1, T):
            both = both + parts[at * T + j].astype(f32)
        both = both.astype(bf16)
        if k == 0:
            low_out[...] = both
        both = both.astype(f32)
        slot = pack[128:, :128].astype(f32)[:1].astype(jnp.int32)
        gs.append(spread(both[:RANK], slot).astype(bf16))
        hs.append(spread(both[RANK:], slot, me[0] * (SLOTS // Y), SLOTS // Y).astype(bf16))
    xs = jnp.concatenate([p[:128, :fx] for p in (p0, p1, p2, p3)], axis=0)
    cs = jnp.concatenate([p[:128, fx:] for p in (p0, p1, p2, p3)], axis=0)
    down = jnp.dot(jnp.concatenate(gs, axis=1), xs, preferred_element_type=f32)
    up = jnp.dot(jnp.concatenate(hs, axis=1), cs, preferred_element_type=f32)
    rd, ru = ROWS // Z, ROWS // Y // Z
    for z in range(Z):
        one = down[z * rd : (z + 1) * rd]
        out[z] = jnp.concatenate([one[:, :128], one[:, 128:], up[z * ru : (z + 1) * ru]], axis=0).astype(bf16)


def finish_kernel(parts, out):
    total = (adapter_scale * jnp.sum(parts[...].astype(f32), axis=0)).astype(bf16)
    for z in range(Z):
        out[z] = total


def layout_kernel(me, g0, g1, g2, g3, down, up):
    rd = ROWS // Z
    for k, g in enumerate((g0, g1, g2, g3)):
        at = me[0] ^ k
        v = g[...].astype(f32)
        down[:, pl.ds(pl.multiple_of(at * 256, 256), 128)] = v[:, :rd].reshape(ROWS, 128).astype(bf16)
        down[:, pl.ds(pl.multiple_of(at * 256 + 128, 128), 128)] = v[:, rd : 2 * rd].reshape(ROWS, 128).astype(bf16)
        up[pl.ds(pl.multiple_of(at * 128, 128), 128)] = v[:, 2 * rd :].reshape(128, 128).astype(bf16)


def frozen_kernel(where, c, w, out):
    out[0] = lax.dot_general(c[...], w[...], NT, preferred_element_type=f32).astype(bf16)


def pair_kernel(kept, came, o0, o1, o2, o3):
    for k, out in enumerate((o0, o1, o2, o3)):
        out[...] = (kept[k].astype(f32) + came[k].astype(f32)).astype(bf16)


def input_kernel(f0, f1, f2, f3, low, slot, down, out):
    g = low[...].astype(f32)[:RANK]
    s = spread(g, slot[:1].astype(jnp.int32)).T.astype(bf16)
    adapter = jnp.dot(s, down[...], preferred_element_type=f32)
    frozen = (f0[...].astype(f32) + f1[...].astype(f32)) + (f2[...].astype(f32) + f3[...].astype(f32))
    out[...] = (frozen + adapter_scale * adapter).astype(bf16)


def swap(value, axis):
    return lax.all_to_all(value, axis, 0, 0, tiled=True)


def trade(value, axis, k):
    return lax.ppermute(value, axis, [(i, i ^ k) for i in range(lax.axis_size(axis))])


def specs(count):
    return [pl.BlockSpec(memory_space=pltpu.SMEM)] + [pl.BlockSpec(memory_space=pltpu.VMEM)] * count


def frozen_blocks(c, w, place):
    n, fc = c.shape
    fx = w.shape[0] // T
    return pl.pallas_call(
        frozen_kernel,
        compiler_params=GRANT,
        grid_spec=pltpu.PrefetchScalarGridSpec(
            num_scalar_prefetch=1,
            grid=(4,),
            in_specs=[
                pl.BlockSpec((n, fc), lambda i, p: (0, 0)),
                pl.BlockSpec((fx, fc), lambda i, p: ((p[0] ^ i) * 2 + p[1], 0)),
            ],
            out_specs=pl.BlockSpec((1, n, fx), lambda i, p: (i, 0, 0)),
        ),
        out_shape=jax.ShapeDtypeStruct((4, n, fx), bf16),
        cost_estimate=pl.CostEstimate(flops=10**9, bytes_accessed=0, transcendentals=0),
    )(place, c, w)


def per_device(x, c, w, down, up, doc, tenant, index):
    n, fx = x.shape
    fc = c.shape[1]
    me = lax.axis_index("y")[None]
    at = lax.axis_index("tensor")
    down_rows = jnp.transpose(down, (0, 2, 1)).reshape(ROWS, fx)
    up_rows = up.reshape(ROWS, fc)
    block = (ROWS // Z * 2 + ROWS // Y // Z, 128)
    part, slot, *packs = call(
        partial_kernel,
        [((Y * T, 2 * RANK, n), bf16), ((8, n), f32)] + [((n + 8, fx // Y + fc), bf16)] * Y,
        flops=10**9,
        grant=pltpu.CompilerParams(),
        in_specs=[pl.BlockSpec(memory_space=pltpu.VMEM)] * 7 + [pl.BlockSpec(memory_space=pltpu.SMEM)],
    )(x, c, down_rows, up_rows, doc[None], tenant[None], index[None], me)
    parts = swap(part, ("y", "tensor"))
    for k in (1, 2, 3):
        packs[k] = trade(packs[k], "y", k)
    piece, low = call(
        gradient_kernel,
        [((Z, *block), bf16), ((2 * RANK, n), bf16)],
        flops=10**9,
        in_specs=specs(5),
    )(me, parts, *packs)
    sums = swap(piece, "z")
    send = frozen_blocks(c, w, jnp.stack([at >> 1, (at & 1) ^ 1]))
    came = trade(send, "tensor", 1)
    kept = frozen_blocks(c, w, jnp.stack([at >> 1, at & 1]))
    pairs = call(pair_kernel, [((n, fx), bf16)] * 4, flops=10**8)(kept, came)
    frozens = [pairs[0]]
    for k in (1, 2, 3):
        frozens.append(trade(pairs[k], "tensor", 2 * k))
    (done,) = call(finish_kernel, [((Z, *block), bf16)], flops=10**8)(sums)
    rows = swap(done, "z")
    (input_gradient,) = call(input_kernel, [((n, fx), bf16)], flops=10**9, out=jax.ShapeDtypeStruct)(*frozens, low, slot, down_rows)
    outs = [rows]
    for k in (1, 2, 3):
        outs.append(trade(rows, "y", k))
    whole, up_whole = call(
        layout_kernel, [((ROWS, fx), bf16), ((ROWS, fc), bf16)], out=jax.ShapeDtypeStruct, in_specs=specs(4)
    )(me, *outs)
    down_gradient = jnp.transpose(whole.reshape(SLOTS, RANK, fx), (0, 2, 1))
    up_gradient = up_whole.reshape(SLOTS, RANK, fc)
    return input_gradient, down_gradient, up_gradient


def solution(mesh):
    grid = Mesh(mesh.devices.reshape(Z, Y, T), ("z", "y", "tensor"))
    dp = ("z", "y")
    in_specs = (
        P(dp, "tensor"),
        P(dp, "tensor"),
        P(None, "tensor"),
        P(None, "tensor", None),
        P(None, None, "tensor"),
        P(dp),
        P(),
        P(),
    )
    out_specs = (P(dp, "tensor"), P(None, "tensor", None), P(None, None, "tensor"))

    return jax.shard_map(per_device, mesh=grid, in_specs=in_specs, out_specs=out_specs, check_vma=False)
```

```python
import jax
import jax.numpy as jnp
from jax import lax
from jax.experimental import pallas as pl
from jax.experimental.pallas import tpu as pltpu
from jax.sharding import Mesh, PartitionSpec as P

adapter_scale = 2.0

Z, Y, T = 16, 4, 8
SLOTS, RANK = 32, 16
ROWS = SLOTS * RANK
bf16, f32 = jnp.bfloat16, jnp.float32
NT = (((1,), (1,)), ((), ()))


GRANT = pltpu.CompilerParams(vmem_limit_bytes=12 << 20)


def call(body, outs, flops=0, grant=GRANT, out=pltpu.VMEM, **kw):
    return pl.pallas_call(
        body,
        compiler_params=grant,
        out_shape=[out(s, d) for s, d in outs],
        cost_estimate=pl.CostEstimate(flops=flops, bytes_accessed=0, transcendentals=0),
        **kw,
    )


def spread(low, slot, first=0, slots=SLOTS):
    at = lax.broadcasted_iota(jnp.int32, (slots * RANK, low.shape[1]), 0) // RANK + first
    return jnp.where(at == slot, jnp.concatenate([low] * slots, axis=0), 0.0)


def partial_kernel(x, c, down, up, doc, tenant, index, me, part, slot_out, *packs):
    n = x.shape[0]
    tenant_of = (lax.broadcasted_iota(jnp.int32, (SLOTS, tenant.shape[1]), 0) == tenant[...]).astype(bf16)
    table = jnp.broadcast_to(index[...].astype(f32), (8, SLOTS)).astype(bf16)
    slot_of_doc = jnp.dot(table, tenant_of, preferred_element_type=f32).astype(bf16)
    doc_of = (lax.broadcasted_iota(jnp.int32, (tenant.shape[1], n), 0) == doc[...]).astype(bf16)
    slot = jnp.dot(slot_of_doc, doc_of, preferred_element_type=f32)
    slot_out[...] = slot
    member = lax.broadcasted_iota(jnp.int32, (ROWS, n), 0) // RANK == slot[:1].astype(jnp.int32)
    h_all = lax.dot_general(down[...], x[...], NT, preferred_element_type=f32)
    g_all = lax.dot_general(up[...], c[...], NT, preferred_element_type=f32)
    g = jnp.sum(jnp.where(member, g_all, 0.0).reshape(SLOTS, RANK, n), axis=0)
    h = jnp.sum(jnp.where(member, h_all, 0.0).reshape(SLOTS, RANK, n), axis=0)
    both = jnp.concatenate([g, h], axis=0)
    for i in range(Y * T):
        part[i] = both
    fx = x.shape[1] // Y
    slots = jnp.concatenate([slot, jnp.zeros((8, fx + c.shape[1] - n), f32)], axis=1)
    for k, pack in enumerate(packs):
        at = pl.multiple_of((me[0] ^ k) * fx, fx)
        mine = jnp.concatenate([x[:, pl.ds(at, fx)], c[...]], axis=1)
        pack[...] = jnp.concatenate([mine.astype(f32), slots], axis=0).astype(bf16)


def gradient_kernel(me, parts, p0, p1, p2, p3, out, low_out):
    fx = p0.shape[1] - 128
    gs, hs = [], []
    for k, pack in enumerate((p0, p1, p2, p3)):
        at = me[0] ^ k
        both = parts[at * T]
        for j in range(1, T):
            both = both + parts[at * T + j]
        both = both.astype(bf16)
        if k == 0:
            low_out[...] = both
        both = both.astype(f32)
        slot = pack[128:, :128].astype(f32)[:1].astype(jnp.int32)
        gs.append(spread(both[:RANK], slot).astype(bf16))
        hs.append(spread(both[RANK:], slot, me[0] * (SLOTS // Y), SLOTS // Y).astype(bf16))
    xs = jnp.concatenate([p[:128, :fx] for p in (p0, p1, p2, p3)], axis=0)
    cs = jnp.concatenate([p[:128, fx:] for p in (p0, p1, p2, p3)], axis=0)
    down = jnp.dot(jnp.concatenate(gs, axis=1), xs, preferred_element_type=f32)
    up = jnp.dot(jnp.concatenate(hs, axis=1), cs, preferred_element_type=f32)
    rd, ru = ROWS // Z, ROWS // Y // Z
    for z in range(Z):
        one = down[z * rd : (z + 1) * rd]
        out[z] = jnp.concatenate([one[:, :128], one[:, 128:], up[z * ru : (z + 1) * ru]], axis=0).astype(bf16)


def finish_kernel(parts, out):
    total = (adapter_scale * jnp.sum(parts[...].astype(f32), axis=0)).astype(bf16)
    for z in range(Z // 2):
        out[z] = total


def layout_kernel(parts, down, up):
    rd = ROWS // Z
    for q in range(2 * Y):
        b, y = q // Y, q % Y
        v = parts[q].astype(f32)
        for k in (0, 1):
            at = y * 256 + k * 128
            down[:, b, :, at : at + 128] = v[:, k * rd : (k + 1) * rd].astype(bf16)
        up[y, :, b] = v[:, 2 * rd :].astype(bf16)


def frozen_kernel(where, c, w, out):
    out[0] = lax.dot_general(c[...], w[...], NT, preferred_element_type=f32).astype(bf16)


def pair_kernel(kept, came, o0, o1, o2, o3):
    for k, out in enumerate((o0, o1, o2, o3)):
        out[...] = (kept[k].astype(f32) + came[k].astype(f32)).astype(bf16)


def input_kernel(f0, f1, f2, f3, low, slot, down, out):
    g = low[...].astype(f32)[:RANK]
    s = spread(g, slot[:1].astype(jnp.int32)).T.astype(bf16)
    adapter = jnp.dot(s, down[...], preferred_element_type=f32)
    frozen = (f0[...].astype(f32) + f1[...].astype(f32)) + (f2[...].astype(f32) + f3[...].astype(f32))
    out[...] = (frozen + adapter_scale * adapter).astype(bf16)


def swap(value, axis):
    return lax.all_to_all(value, axis, 0, 0, tiled=True)


def trade(value, axis, k):
    return lax.ppermute(value, axis, [(i, i ^ k) for i in range(lax.axis_size(axis))])


def to_all(value, axes):
    count = lax.axis_size(axes)
    return swap(jnp.broadcast_to(value[None], (count, *value.shape)), axes)


def specs(count):
    return [pl.BlockSpec(memory_space=pltpu.SMEM)] + [pl.BlockSpec(memory_space=pltpu.VMEM)] * count


def frozen_blocks(c, w, place):
    n, fc = c.shape
    fx = w.shape[0] // T
    return pl.pallas_call(
        frozen_kernel,
        compiler_params=GRANT,
        grid_spec=pltpu.PrefetchScalarGridSpec(
            num_scalar_prefetch=1,
            grid=(4,),
            in_specs=[
                pl.BlockSpec((n, fc), lambda i, p: (0, 0)),
                pl.BlockSpec((fx, fc), lambda i, p: ((p[0] ^ i) * 2 + p[1], 0)),
            ],
            out_specs=pl.BlockSpec((1, n, fx), lambda i, p: (i, 0, 0)),
        ),
        out_shape=jax.ShapeDtypeStruct((4, n, fx), bf16),
        cost_estimate=pl.CostEstimate(flops=10**9, bytes_accessed=0, transcendentals=0),
    )(place, c, w)


def per_device(x, c, w, down, up, doc, tenant, index):
    n, fx = x.shape
    fc = c.shape[1]
    me = lax.axis_index("y")[None]
    at = lax.axis_index("tensor")
    down_rows = jnp.transpose(down, (0, 2, 1)).reshape(ROWS, fx)
    up_rows = up.reshape(ROWS, fc)
    block = (ROWS // Z * 2 + ROWS // Y // Z, 128)
    part, slot, *packs = call(
        partial_kernel,
        [((Y * T, 2 * RANK, n), f32), ((8, n), f32)] + [((n + 8, fx // Y + fc), bf16)] * Y,
        flops=10**9,
        grant=pltpu.CompilerParams(),
        in_specs=[pl.BlockSpec(memory_space=pltpu.VMEM)] * 7 + [pl.BlockSpec(memory_space=pltpu.SMEM)],
    )(x, c, down_rows, up_rows, doc[None], tenant[None], index[None], me)
    parts = swap(part, ("y", "tensor"))
    for k in (1, 2, 3):
        packs[k] = trade(packs[k], "y", k)
    piece, low = call(
        gradient_kernel,
        [((Z, *block), bf16), ((2 * RANK, n), bf16)],
        flops=10**9,
        in_specs=specs(5),
    )(me, parts, *packs)
    sums = swap(piece, ("zh", "zl"))
    send = frozen_blocks(c, w, jnp.stack([at >> 1, (at & 1) ^ 1]))
    came = trade(send, "tensor", 1)
    kept = frozen_blocks(c, w, jnp.stack([at >> 1, at & 1]))
    pairs = call(pair_kernel, [((n, fx), bf16)] * 4, flops=10**8)(kept, came)
    frozens = [pairs[0]]
    for k in (1, 2, 3):
        frozens.append(trade(pairs[k], "tensor", 2 * k))
    (done,) = call(finish_kernel, [((Z // 2, *block), bf16)], flops=10**8)(sums)
    rows = swap(done, "zh")
    (input_gradient,) = call(input_kernel, [((n, fx), bf16)], flops=10**9, out=jax.ShapeDtypeStruct)(*frozens, low, slot, down_rows)
    outs = to_all(rows, ("zl", "y"))
    whole, up_whole = call(
        layout_kernel,
        [((Z // 2, 2, ROWS // Z, fx), bf16), ((Y, Z // 2, 2, ROWS // Y // Z, fc), bf16)],
        out=jax.ShapeDtypeStruct,
    )(outs)
    down_gradient = jnp.transpose(whole.reshape(SLOTS, RANK, fx), (0, 2, 1))
    up_gradient = up_whole.reshape(SLOTS, RANK, fc)
    return input_gradient, down_gradient, up_gradient


def solution(mesh):
    grid = Mesh(mesh.devices.reshape(Z // 2, 2, Y, T), ("zh", "zl", "y", "tensor"))
    dp = ("zh", "zl", "y")
    in_specs = (
        P(dp, "tensor"),
        P(dp, "tensor"),
        P(None, "tensor"),
        P(None, "tensor", None),
        P(None, None, "tensor"),
        P(dp),
        P(),
        P(),
    )
    out_specs = (P(dp, "tensor"), P(None, "tensor", None), P(None, None, "tensor"))

    return jax.shard_map(per_device, mesh=grid, in_specs=in_specs, out_specs=out_specs, check_vma=False)
```

```python
import jax
import jax.numpy as jnp
from jax import lax
from jax.experimental import pallas as pl
from jax.experimental.pallas import tpu as pltpu
from jax.sharding import Mesh, PartitionSpec as P

adapter_scale = 2.0

Z, Y, T = 16, 4, 8
SLOTS, RANK = 32, 16
ROWS = SLOTS * RANK
bf16, f32 = jnp.bfloat16, jnp.float32
NT = (((1,), (1,)), ((), ()))


GRANT = pltpu.CompilerParams(vmem_limit_bytes=12 << 20)


def call(body, outs, flops=0, grant=GRANT, out=pltpu.VMEM, **kw):
    return pl.pallas_call(
        body,
        compiler_params=grant,
        out_shape=[out(s, d) for s, d in outs],
        cost_estimate=pl.CostEstimate(flops=flops, bytes_accessed=0, transcendentals=0),
        **kw,
    )


def spread(low, slot, first=0, slots=SLOTS):
    at = lax.broadcasted_iota(jnp.int32, (slots * RANK, low.shape[1]), 0) // RANK + first
    return jnp.where(at == slot, jnp.concatenate([low] * slots, axis=0), 0.0)


def partial_kernel(x, c, down, up, doc, tenant, index, part, slot_out, pack):
    n = x.shape[0]
    tenant_of = (lax.broadcasted_iota(jnp.int32, (SLOTS, tenant.shape[1]), 0) == tenant[...]).astype(bf16)
    table = jnp.broadcast_to(index[...].astype(f32), (8, SLOTS)).astype(bf16)
    slot_of_doc = jnp.dot(table, tenant_of, preferred_element_type=f32).astype(bf16)
    doc_of = (lax.broadcasted_iota(jnp.int32, (tenant.shape[1], n), 0) == doc[...]).astype(bf16)
    slot = jnp.dot(slot_of_doc, doc_of, preferred_element_type=f32)
    slot_out[...] = slot
    member = lax.broadcasted_iota(jnp.int32, (ROWS, n), 0) // RANK == slot[:1].astype(jnp.int32)
    h_all = lax.dot_general(down[...], x[...], NT, preferred_element_type=f32)
    g_all = lax.dot_general(up[...], c[...], NT, preferred_element_type=f32)
    g = jnp.sum(jnp.where(member, g_all, 0.0).reshape(SLOTS, RANK, n), axis=0)
    h = jnp.sum(jnp.where(member, h_all, 0.0).reshape(SLOTS, RANK, n), axis=0)
    both = jnp.concatenate([g, h], axis=0)
    for i in range(Y * T):
        part[i] = both
    fx = x.shape[1] // Y
    slots = jnp.concatenate([slot, jnp.zeros((8, fx + c.shape[1] - n), f32)], axis=1)
    for y in range(Y):
        mine = jnp.concatenate([x[:, y * fx : (y + 1) * fx], c[...]], axis=1)
        pack[y] = jnp.concatenate([mine.astype(f32), slots], axis=0).astype(bf16)


def gradient_kernel(me, parts, packs, out, low_out):
    fx = packs.shape[2] - 128
    gs, hs = [], []
    for y in range(Y):
        both = parts[y * T]
        for j in range(1, T):
            both = both + parts[y * T + j]
        both = both.astype(bf16)

        @pl.when(me[0] == y)
        def _():
            low_out[...] = both

        both = both.astype(f32)
        slot = packs[y, 128:, :128].astype(f32)[:1].astype(jnp.int32)
        gs.append(spread(both[:RANK], slot).astype(bf16))
        hs.append(spread(both[RANK:], slot, me[0] * (SLOTS // Y), SLOTS // Y).astype(bf16))
    xs = jnp.concatenate([packs[y, :128, :fx] for y in range(Y)], axis=0)
    cs = jnp.concatenate([packs[y, :128, fx:] for y in range(Y)], axis=0)
    down = jnp.dot(jnp.concatenate(gs, axis=1), xs, preferred_element_type=f32)
    up = jnp.dot(jnp.concatenate(hs, axis=1), cs, preferred_element_type=f32)
    rd, ru = ROWS // Z, ROWS // Y // Z
    for z in range(Z):
        one = down[z * rd : (z + 1) * rd]
        out[z] = jnp.concatenate([one[:, :128], one[:, 128:], up[z * ru : (z + 1) * ru]], axis=0).astype(bf16)


def finish_kernel(parts, out):
    total = (adapter_scale * jnp.sum(parts[...].astype(f32), axis=0)).astype(bf16)
    for z in range(Z):
        out[z] = total


def layout_kernel(parts, down, up):
    rd = ROWS // Z
    for y in range(Y):
        v = parts[y].astype(f32)
        for k in (0, 1):
            at = y * 256 + k * 128
            down[:, at : at + 128] = v[:, k * rd : (k + 1) * rd].reshape(ROWS, 128).astype(bf16)
        up[y * 128 : (y + 1) * 128] = v[:, 2 * rd :].reshape(128, 128).astype(bf16)


def frozen_kernel(where, c, w, out):
    out[0] = lax.dot_general(c[...], w[...], NT, preferred_element_type=f32).astype(bf16)


def pair_kernel(kept, came, o0, o1, o2, o3):
    for k, out in enumerate((o0, o1, o2, o3)):
        out[...] = (kept[k].astype(f32) + came[k].astype(f32)).astype(bf16)


def input_kernel(f0, f1, f2, f3, low, slot, down, out):
    g = low[...].astype(f32)[:RANK]
    s = spread(g, slot[:1].astype(jnp.int32)).T.astype(bf16)
    adapter = jnp.dot(s, down[...], preferred_element_type=f32)
    frozen = (f0[...].astype(f32) + f1[...].astype(f32)) + (f2[...].astype(f32) + f3[...].astype(f32))
    out[...] = (frozen + adapter_scale * adapter).astype(bf16)


def swap(value, axis):
    return lax.all_to_all(value, axis, 0, 0, tiled=True)


def trade(value, axis, k):
    return lax.ppermute(value, axis, [(i, i ^ k) for i in range(lax.axis_size(axis))])


def to_all(value, axes):
    count = lax.axis_size(axes)
    return swap(jnp.broadcast_to(value[None], (count, *value.shape)), axes)


def specs(count):
    return [pl.BlockSpec(memory_space=pltpu.SMEM)] + [pl.BlockSpec(memory_space=pltpu.VMEM)] * count


def frozen_blocks(c, w, place):
    n, fc = c.shape
    fx = w.shape[0] // T
    return pl.pallas_call(
        frozen_kernel,
        compiler_params=GRANT,
        grid_spec=pltpu.PrefetchScalarGridSpec(
            num_scalar_prefetch=1,
            grid=(4,),
            in_specs=[
                pl.BlockSpec((n, fc), lambda i, p: (0, 0)),
                pl.BlockSpec((fx, fc), lambda i, p: ((p[0] ^ i) * 2 + p[1], 0)),
            ],
            out_specs=pl.BlockSpec((1, n, fx), lambda i, p: (i, 0, 0)),
        ),
        out_shape=jax.ShapeDtypeStruct((4, n, fx), bf16),
        cost_estimate=pl.CostEstimate(flops=10**9, bytes_accessed=0, transcendentals=0),
    )(place, c, w)


def per_device(x, c, w, down, up, doc, tenant, index):
    n, fx = x.shape
    fc = c.shape[1]
    me = lax.axis_index("y")[None]
    at = lax.axis_index("tensor")
    mine, other = at & 1, (at & 1) ^ 1
    column = at >> 1
    down_rows = jnp.transpose(down, (0, 2, 1)).reshape(ROWS, fx)
    up_rows = up.reshape(ROWS, fc)
    block = (ROWS // Z * 2 + ROWS // Y // Z, 128)
    part, slot, pack = call(
        partial_kernel,
        [((Y * T, 2 * RANK, n), f32), ((8, n), f32), ((Y, n + 8, fx // Y + fc), bf16)],
        flops=10**9,
        grant=pltpu.CompilerParams(),
    )(x, c, down_rows, up_rows, doc[None], tenant[None], index[None])
    parts = swap(part, ("y", "tensor"))
    packs = swap(pack, "y")
    piece, low = call(
        gradient_kernel,
        [((Z, *block), bf16), ((2 * RANK, n), bf16)],
        flops=10**9,
        in_specs=specs(2),
    )(me, parts, packs)
    sums = swap(piece, "z")
    to_send, to_keep = jnp.stack([column, other]), jnp.stack([column, mine])
    send = frozen_blocks(c, w, to_send)
    came = trade(send, "tensor", 1)
    kept = frozen_blocks(c, w, to_keep)
    pairs = call(pair_kernel, [((n, fx), bf16)] * 4, flops=10**8)(kept, came)
    frozens = [pairs[0]]
    for k in (1, 2, 3):
        frozens.append(trade(pairs[k], "tensor", 2 * k))
    (done,) = call(finish_kernel, [((Z, *block), bf16)], flops=10**8)(sums)
    rows = swap(done, "z")
    (input_gradient,) = call(input_kernel, [((n, fx), bf16)], flops=10**9, out=jax.ShapeDtypeStruct)(*frozens, low, slot, down_rows)
    outs = to_all(rows, "y")
    whole, up_whole = call(
        layout_kernel,
        [((ROWS, fx), bf16), ((ROWS, fc), bf16)],
        out=jax.ShapeDtypeStruct,
    )(outs)
    down_gradient = jnp.transpose(whole.reshape(SLOTS, RANK, fx), (0, 2, 1))
    up_gradient = up_whole.reshape(SLOTS, RANK, fc)
    return input_gradient, down_gradient, up_gradient


def solution(mesh):
    grid = Mesh(mesh.devices.reshape(Z, Y, T), ("z", "y", "tensor"))
    dp = ("z", "y")
    in_specs = (
        P(dp, "tensor"),
        P(dp, "tensor"),
        P(None, "tensor"),
        P(None, "tensor", None),
        P(None, None, "tensor"),
        P(dp),
        P(),
        P(),
    )
    out_specs = (P(dp, "tensor"), P(None, "tensor", None), P(None, None, "tensor"))

    return jax.shard_map(per_device, mesh=grid, in_specs=in_specs, out_specs=out_specs, check_vma=False)
```

```python
import jax
import jax.numpy as jnp
from jax import lax
from jax.experimental import pallas as pl
from jax.experimental.pallas import tpu as pltpu
from jax.sharding import Mesh, PartitionSpec as P

adapter_scale = 2.0

Z, Y, T = 16, 4, 8
SLOTS, RANK = 32, 16
ROWS = SLOTS * RANK
bf16, f32 = jnp.bfloat16, jnp.float32
NT = (((1,), (1,)), ((), ()))


GRANT = pltpu.CompilerParams(vmem_limit_bytes=12 << 20)


def call(body, outs, flops=0, grant=GRANT, out=pltpu.VMEM, **kw):
    return pl.pallas_call(
        body,
        compiler_params=grant,
        out_shape=[out(s, d) for s, d in outs],
        cost_estimate=pl.CostEstimate(flops=flops, bytes_accessed=0, transcendentals=0),
        **kw,
    )


def spread(low, slot, first=0, slots=SLOTS):
    at = lax.broadcasted_iota(jnp.int32, (slots * RANK, low.shape[1]), 0) // RANK + first
    return jnp.where(at == slot, jnp.concatenate([low] * slots, axis=0), 0.0)


def token_kernel(x, c, doc, tenant, index, me, slot_out, *packs):
    n = x.shape[0]
    tenant_of = (lax.broadcasted_iota(jnp.int32, (SLOTS, tenant.shape[1]), 0) == tenant[...]).astype(bf16)
    table = jnp.broadcast_to(index[...].astype(f32), (8, SLOTS)).astype(bf16)
    slot_of_doc = jnp.dot(table, tenant_of, preferred_element_type=f32).astype(bf16)
    doc_of = (lax.broadcasted_iota(jnp.int32, (tenant.shape[1], n), 0) == doc[...]).astype(bf16)
    slot = jnp.dot(slot_of_doc, doc_of, preferred_element_type=f32)
    slot_out[...] = slot
    fx = x.shape[1] // Y
    slots = jnp.concatenate([slot, jnp.zeros((8, fx + c.shape[1] - n), f32)], axis=1)
    for k, pack in enumerate(packs):
        at = pl.multiple_of((me[0] ^ k) * fx, fx)
        mine = jnp.concatenate([x[:, pl.ds(at, fx)], c[...]], axis=1)
        pack[...] = jnp.concatenate([mine.astype(f32), slots], axis=0).astype(bf16)


def partial_kernel(x_in, c_in, down_in, up_in, slot, part, x, c, down, up, sems):
    loads = [
        pltpu.make_async_copy(source, target, sems.at[i])
        for i, (source, target) in enumerate(((down_in, down), (x_in, x), (up_in, up), (c_in, c)))
    ]
    for load in loads:
        load.start()
    for load in loads:
        load.wait()
    n = x.shape[0]
    member = lax.broadcasted_iota(jnp.int32, (ROWS, n), 0) // RANK == slot[:1].astype(jnp.int32)
    h_all = lax.dot_general(down[...], x[...], NT, preferred_element_type=f32)
    g_all = lax.dot_general(up[...], c[...], NT, preferred_element_type=f32)
    g = jnp.sum(jnp.where(member, g_all, 0.0).reshape(SLOTS, RANK, n), axis=0)
    h = jnp.sum(jnp.where(member, h_all, 0.0).reshape(SLOTS, RANK, n), axis=0)
    both = jnp.concatenate([g, h], axis=0).astype(bf16)
    for i in range(Y * T):
        part[i] = both


def gradient_kernel(me, parts, p0, p1, p2, p3, out, low_out):
    fx = p0.shape[1] - 128
    gs, hs = [], []
    for k, pack in enumerate((p0, p1, p2, p3)):
        at = me[0] ^ k
        both = parts[at * T].astype(f32)
        for j in range(1, T):
            both = both + parts[at * T + j].astype(f32)
        both = both.astype(bf16)
        if k == 0:
            low_out[...] = both
        both = both.astype(f32)
        slot = pack[128:, :128].astype(f32)[:1].astype(jnp.int32)
        gs.append(spread(both[:RANK], slot).astype(bf16))
        hs.append(spread(both[RANK:], slot, me[0] * (SLOTS // Y), SLOTS // Y).astype(bf16))
    xs = jnp.concatenate([p[:128, :fx] for p in (p0, p1, p2, p3)], axis=0)
    cs = jnp.concatenate([p[:128, fx:] for p in (p0, p1, p2, p3)], axis=0)
    down = jnp.dot(jnp.concatenate(gs, axis=1), xs, preferred_element_type=f32)
    up = jnp.dot(jnp.concatenate(hs, axis=1), cs, preferred_element_type=f32)
    rd, ru = ROWS // Z, ROWS // Y // Z
    for z in range(Z):
        one = down[z * rd : (z + 1) * rd]
        out[z] = jnp.concatenate([one[:, :128], one[:, 128:], up[z * ru : (z + 1) * ru]], axis=0).astype(bf16)


def finish_kernel(parts, out):
    total = (adapter_scale * jnp.sum(parts[...].astype(f32), axis=0)).astype(bf16)
    for z in range(Z // 2):
        out[z] = total


def layout_kernel(parts, down, up):
    rd = ROWS // Z
    for q in range(2 * Y):
        b, y = q // Y, q % Y
        v = parts[q].astype(f32)
        for k in (0, 1):
            at = y * 256 + k * 128
            down[:, b, :, at : at + 128] = v[:, k * rd : (k + 1) * rd].astype(bf16)
        up[y, :, b] = v[:, 2 * rd :].astype(bf16)


def frozen_kernel(where, c, w, out):
    out[0] = lax.dot_general(c[...], w[...], NT, preferred_element_type=f32).astype(bf16)


def pair_kernel(kept, came, o0, o1, o2, o3):
    for k, out in enumerate((o0, o1, o2, o3)):
        out[...] = (kept[k].astype(f32) + came[k].astype(f32)).astype(bf16)


def input_kernel(f0, f1, f2, f3, low, slot, down, out):
    g = low[...].astype(f32)[:RANK]
    s = spread(g, slot[:1].astype(jnp.int32)).T.astype(bf16)
    adapter = jnp.dot(s, down[...], preferred_element_type=f32)
    frozen = (f0[...].astype(f32) + f1[...].astype(f32)) + (f2[...].astype(f32) + f3[...].astype(f32))
    out[...] = (frozen + adapter_scale * adapter).astype(bf16)


def swap(value, axis):
    return lax.all_to_all(value, axis, 0, 0, tiled=True)


def trade(value, axis, k):
    return lax.ppermute(value, axis, [(i, i ^ k) for i in range(lax.axis_size(axis))])


def to_all(value, axes):
    count = lax.axis_size(axes)
    return swap(jnp.broadcast_to(value[None], (count, *value.shape)), axes)


def specs(count):
    return [pl.BlockSpec(memory_space=pltpu.SMEM)] + [pl.BlockSpec(memory_space=pltpu.VMEM)] * count


def frozen_blocks(c, w, place):
    n, fc = c.shape
    fx = w.shape[0] // T
    return pl.pallas_call(
        frozen_kernel,
        compiler_params=GRANT,
        grid_spec=pltpu.PrefetchScalarGridSpec(
            num_scalar_prefetch=1,
            grid=(4,),
            in_specs=[
                pl.BlockSpec((n, fc), lambda i, p: (0, 0)),
                pl.BlockSpec((fx, fc), lambda i, p: ((p[0] ^ i) * 2 + p[1], 0)),
            ],
            out_specs=pl.BlockSpec((1, n, fx), lambda i, p: (i, 0, 0)),
        ),
        out_shape=jax.ShapeDtypeStruct((4, n, fx), bf16),
        cost_estimate=pl.CostEstimate(flops=10**9, bytes_accessed=0, transcendentals=0),
    )(place, c, w)


def per_device(x, c, w, down, up, doc, tenant, index):
    n, fx = x.shape
    fc = c.shape[1]
    me = lax.axis_index("y")[None]
    at = lax.axis_index("tensor")
    down_rows = jnp.transpose(down, (0, 2, 1)).reshape(ROWS, fx)
    up_rows = up.reshape(ROWS, fc)
    block = (ROWS // Z * 2 + ROWS // Y // Z, 128)
    slot, *packs = call(
        token_kernel,
        [((8, n), f32)] + [((n + 8, fx // Y + fc), bf16)] * Y,
        flops=10**8,
        grant=pltpu.CompilerParams(),
        out=jax.ShapeDtypeStruct,
        in_specs=[pl.BlockSpec(memory_space=pltpu.VMEM)] * 5 + [pl.BlockSpec(memory_space=pltpu.SMEM)],
    )(x, c, doc[None], tenant[None], index[None], me)
    (part,) = call(
        partial_kernel,
        [((Y * T, 2 * RANK, n), bf16)],
        flops=10**9,
        in_specs=[pl.BlockSpec(memory_space=pltpu.HBM)] * 4 + [pl.BlockSpec(memory_space=pltpu.VMEM)],
        scratch_shapes=[
            pltpu.VMEM((n, fx), bf16),
            pltpu.VMEM((n, fc), bf16),
            pltpu.VMEM((ROWS, fx), bf16),
            pltpu.VMEM((ROWS, fc), bf16),
            pltpu.SemaphoreType.DMA((4,)),
        ],
    )(*(pltpu.with_memory_space_constraint(v, pltpu.HBM) for v in (x, c, down_rows, up_rows)), slot)
    parts = swap(part, ("y", "tensor"))
    for k in (1, 2, 3):
        packs[k] = trade(packs[k], "y", k)
    piece, low = call(
        gradient_kernel,
        [((Z, *block), bf16), ((2 * RANK, n), bf16)],
        flops=10**9,
        in_specs=specs(5),
    )(me, parts, *packs)
    sums = swap(piece, ("zh", "zl"))
    send = frozen_blocks(c, w, jnp.stack([at >> 1, (at & 1) ^ 1]))
    came = trade(send, "tensor", 1)
    kept = frozen_blocks(c, w, jnp.stack([at >> 1, at & 1]))
    pairs = call(pair_kernel, [((n, fx), bf16)] * 4, flops=10**8)(kept, came)
    frozens = [pairs[0]]
    for k in (1, 2, 3):
        frozens.append(trade(pairs[k], "tensor", 2 * k))
    (done,) = call(finish_kernel, [((Z // 2, *block), bf16)], flops=10**8)(sums)
    rows = swap(done, "zh")
    (input_gradient,) = call(input_kernel, [((n, fx), bf16)], flops=10**9, out=jax.ShapeDtypeStruct)(*frozens, low, slot, down_rows)
    outs = to_all(rows, ("zl", "y"))
    whole, up_whole = call(
        layout_kernel,
        [((Z // 2, 2, ROWS // Z, fx), bf16), ((Y, Z // 2, 2, ROWS // Y // Z, fc), bf16)],
        out=jax.ShapeDtypeStruct,
    )(outs)
    down_gradient = jnp.transpose(whole.reshape(SLOTS, RANK, fx), (0, 2, 1))
    up_gradient = up_whole.reshape(SLOTS, RANK, fc)
    return input_gradient, down_gradient, up_gradient


def solution(mesh):
    grid = Mesh(mesh.devices.reshape(Z // 2, 2, Y, T), ("zh", "zl", "y", "tensor"))
    dp = ("zh", "zl", "y")
    in_specs = (
        P(dp, "tensor"),
        P(dp, "tensor"),
        P(None, "tensor"),
        P(None, "tensor", None),
        P(None, None, "tensor"),
        P(dp),
        P(),
        P(),
    )
    out_specs = (P(dp, "tensor"), P(None, "tensor", None), P(None, None, "tensor"))

    return jax.shard_map(per_device, mesh=grid, in_specs=in_specs, out_specs=out_specs, check_vma=False)
```
